32 devices in a mesh: section: 8 (over z, x), seq: 4 (over y, core).
Axes of the slice: x: 2, y: 2, z: 4, core: 2. Of those that a mesh axis runs over, the one named last changes fastest.
Arguments:
- held_q: bfloat16 [8, 256, 4096], P('section', None, 'seq'), may hold values from -200 to 200
- held_kv: bfloat16 [8, 256, 4, 256], P('section'), may hold values from -30 to 30
- grad_out: bfloat16 [8, 256, 4096], P('section', None, 'seq'), may hold values from -6 to 6
Outputs:
- grad_q: bfloat16 [8, 256, 4096], P('section', 'seq')
- grad_kv: bfloat16 [8, 256, 4, 256], P('section', 'seq')
The draws below stay inside these ranges and needn't reach their ends.
All inputs are finite; a program needn't handle non-finite values.
Results may differ from the reference program's by a relative error of at most 0.01.
Values may be sent and summed in bfloat16 or wider, within the bound.
A program may use at most 64 MiB of HBM per device.

```python
import jax
import jax.numpy as jnp
from jax import lax

HD = 128
KVH = 4
GROUP = 8
QH = 32
SPAN = 256
N_SECTION = 8
N_SEQ = 4


def draw_held_q(key, part):
    base = jnp.clip(jax.random.normal(jax.random.fold_in(key, 1), (N_SECTION, SPAN, QH, HD), jnp.float32), -6.0, 6.0)
    return base.reshape(N_SECTION, SPAN, QH * HD).astype(jnp.bfloat16)


def draw_held_kv(key, part):
    key_part = jnp.clip(jax.random.normal(jax.random.fold_in(key, 3), (N_SECTION, SPAN, KVH, HD), jnp.float32), -6.0, 6.0)
    value_part = jnp.clip(jax.random.normal(jax.random.fold_in(key, 4), (N_SECTION, SPAN, KVH, HD), jnp.float32), -6.0, 6.0)
    return jnp.concatenate([key_part, value_part], axis=3).astype(jnp.bfloat16)


def block_scale(own_key, dims, shards, low, top_value):
    def one(dim, blocks):
        steps = jax.random.uniform(jax.random.fold_in(jax.random.fold_in(own_key, 6), dim), (blocks,), jnp.float32, low / len(shards), top_value / len(shards))
        return jnp.repeat(jnp.exp(steps), dims[dim] // blocks).reshape((-1,) + (1,) * (len(dims) - dim - 1))

    loudness = one(*shards[0])
    for cut in shards[1:]:
        loudness = loudness * one(*cut)
    return loudness


def normal_values(stream_key, shape, scale, reach, cuts=(), kind=jnp.bfloat16):
    factor_of = block_scale(stream_key, shape, cuts, -0.22, 0.18) if cuts else 1.0
    drawn = jax.random.normal(stream_key, shape, jnp.float32) * scale * factor_of
    return jnp.minimum(jnp.maximum(drawn, -reach), reach).astype(kind)


def setup_inputs(seed: int = 0) -> dict:
    splits = jax.random.split(jax.random.key(seed), 4)
    return {
        "held_q": draw_held_q(jax.random.fold_in(splits[3], 71), 0),
        "held_kv": draw_held_kv(jax.random.fold_in(splits[3], 71), 0),
        "grad_out": normal_values(splits[2], (N_SECTION, SPAN, QH * HD), 1.0, 6.0, ((0, 8), (2, 4))),
    }


def head_grads(query_head, grad_head, key_rows, value_rows):
    span_len = query_head.shape[0]
    head_dim = query_head.shape[1]
    score_scale = head_dim ** -0.5
    row_pos = lax.broadcasted_iota(jnp.int32, (span_len, span_len), 0)
    col_pos = lax.broadcasted_iota(jnp.int32, (span_len, span_len), 1)
    raw_scores = jnp.dot(query_head, key_rows.T, preferred_element_type=jnp.float32) * score_scale
    scores = jnp.where(col_pos <= row_pos, raw_scores, -1e30)
    row_max = jnp.max(scores, axis=1, keepdims=True)
    expanded = jnp.exp(scores - row_max)
    probs = expanded / jnp.sum(expanded, axis=1, keepdims=True)
    grad_probs = jnp.dot(grad_head, value_rows.T, preferred_element_type=jnp.float32)
    row_dot = jnp.sum(probs * grad_probs, axis=1, keepdims=True)
    grad_scores = (probs * (grad_probs - row_dot)).astype(jnp.bfloat16)
    weights = probs.astype(jnp.bfloat16)
    grad_query = jnp.dot(grad_scores, key_rows, preferred_element_type=jnp.float32) * score_scale
    grad_key = jnp.dot(grad_scores.T, query_head, preferred_element_type=jnp.float32) * score_scale
    grad_value = jnp.dot(weights.T, grad_head, preferred_element_type=jnp.float32)
    return grad_query, grad_key, grad_value


def section_grads(items):
    query_all, pair_all, grad_all = items
    query_heads = query_all.reshape(SPAN, QH, HD).transpose(1, 0, 2)
    grad_heads = grad_all.reshape(SPAN, QH, HD).transpose(1, 0, 2)
    head_ids = jnp.arange(QH, dtype=jnp.int32)

    def one_head(head_items):
        head_num, query_head, grad_head = head_items
        pair_rows = lax.dynamic_index_in_dim(pair_all, (head_num // GROUP).astype(jnp.int32), 1, keepdims=False)
        return head_grads(query_head, grad_head, pair_rows[:, :HD], pair_rows[:, HD:])

    grad_query, grad_key, grad_value = lax.map(one_head, (head_ids, query_heads, grad_heads))
    grad_query = grad_query.astype(jnp.bfloat16).transpose(1, 0, 2).reshape(SPAN, QH * HD)
    per_device = QH // N_SEQ
    repeats = N_SEQ // KVH
    part_key = grad_key.reshape(N_SEQ, per_device, SPAN, HD).sum(axis=1).astype(jnp.bfloat16)
    part_value = grad_value.reshape(N_SEQ, per_device, SPAN, HD).sum(axis=1).astype(jnp.bfloat16)
    key_total = part_key.astype(jnp.float32).reshape(KVH, repeats, SPAN, HD).sum(axis=1).astype(jnp.bfloat16)
    value_total = part_value.astype(jnp.float32).reshape(KVH, repeats, SPAN, HD).sum(axis=1).astype(jnp.bfloat16)
    grad_pair = jnp.concatenate([key_total, value_total], axis=2).transpose(1, 0, 2)
    return grad_query, grad_pair


def reference(held_q, held_kv, grad_out):
    own_q = jnp.roll(held_q, -(N_SECTION // 2), axis=0)
    own_kv = jnp.roll(held_kv, -(N_SECTION // 2), axis=0)
    grad_q, grad_kv = lax.map(section_grads, (own_q, own_kv, grad_out))
    return grad_q, grad_kv
```

```python
import functools
import math

import jax
import jax.numpy as jnp
from jax import lax
from jax.experimental import pallas as pl
from jax.experimental.pallas import tpu as pltpu
from jax.sharding import PartitionSpec as P

MESH = pl.DeviceIdType.MESH
AHEAD = 4


def dot_last(left, right):
    return lax.dot_general(
        left, right, (((1,), (1,)), ((), ())), preferred_element_type=jnp.float32
    )


def dot_plain(left, right):
    return jnp.dot(left, right, preferred_element_type=jnp.float32)


def kernel(
    n_section,
    n_seq,
    kv_heads,
    head_dim,
    heads,
    block_len,
    held_q,
    held_kv,
    grad_out,
    out_q,
    out_kv,
    q_land,
    kv_all,
    kv_send,
    kv_land,
    g_land,
    key_t,
    dk_acc,
    dv_acc,
    gq_buf,
    kvp_buf,
    kv_slots,
    q_send_sem,
    q_recv_sem,
    kv_send_sem,
    kv_recv_sem,
    g_sem,
    load_sem,
    gq_send_sem,
    gq_recv_sem,
    kvp_send_sem,
    kvp_recv_sem,
    door,
):
    section = lax.axis_index("section")
    me = lax.axis_index("seq")
    partner = lax.rem(section + n_section // 2, n_section)
    repeats = n_seq // kv_heads
    own_head = me // repeats
    span = held_q.shape[0]
    tokens = span // n_seq
    scale = head_dim**-0.5

    kv_load = pltpu.make_async_copy(held_kv, kv_all, load_sem)
    kv_load.start()

    def whole(ref, sem):
        return pltpu.make_async_copy(ref, ref, sem)

    def grad_load(h):
        cols = pl.ds(pl.multiple_of(h * head_dim, head_dim), head_dim)
        return pltpu.make_async_copy(grad_out.at[:, cols], g_land.at[h], g_sem)

    edges = sorted({0, tokens, span}, reverse=True)
    parts = list(zip(edges[1:], edges[:-1]))
    last = heads - 1

    def q_copy(h, part=None):
        cols = pl.ds(pl.multiple_of(h * head_dim, head_dim), head_dim)
        rows = slice(0, span) if part is None else slice(*parts[part])
        slot = h if part is None else last + part
        return pltpu.make_async_remote_copy(
            src_ref=held_q.at[rows, cols],
            dst_ref=q_land.at[h, rows, :],
            send_sem=q_send_sem,
            recv_sem=q_recv_sem.at[slot],
            device_id=(partner, me),
            device_id_type=MESH,
        )

    kv_copy = pltpu.make_async_remote_copy(
        src_ref=kv_send,
        dst_ref=kv_land,
        send_sem=kv_send_sem,
        recv_sem=kv_recv_sem,
        device_id=(partner, me),
        device_id_type=MESH,
    )

    def send_unit(unit):
        @pl.when(unit < last)
        def _():
            q_copy(unit).start()

        @pl.when(unit == last)
        def _():
            for part in range(len(parts)):
                q_copy(last, part).start()

    barrier = pltpu.get_barrier_semaphore()
    pl.semaphore_signal(barrier, inc=1, device_id=(partner, me), device_id_type=MESH)
    late = section >= n_section // 2
    early = jnp.logical_not(late)

    def signal_peers(sem):
        for d in range(1, n_seq):
            peer = lax.rem(me + d, n_seq)
            pl.semaphore_signal(
                sem, inc=1, device_id=(section, peer), device_id_type=MESH
            )

    @pl.when(early)
    def _():
        signal_peers(barrier)

    for h in range(heads):
        grad_load(h).start()
    dk_acc[...] = jnp.zeros_like(dk_acc)
    dv_acc[...] = jnp.zeros_like(dv_acc)
    pl.semaphore_wait(barrier, jnp.where(early, n_seq, 1))
    send_unit(0)
    kv_load.wait()
    for j in range(kv_heads):

        @pl.when(own_head == j)
        def _():
            kv_send[...] = kv_all[:, j, :]

    kv_copy.start()
    ahead = jnp.where(section >= n_section - n_section // 4, AHEAD, heads)

    def first_sends(unit, carry):
        @pl.when(unit < ahead)
        def _():
            send_unit(unit)

        return carry

    lax.fori_loop(1, heads, first_sends, 0)

    @pl.when(early)
    def _():
        signal_peers(door)
        pl.semaphore_wait(door, n_seq - 1)
        pl.semaphore_signal(door, inc=1, device_id=(partner, me), device_id_type=MESH)

    @pl.when(late)
    def _():
        pl.semaphore_wait(door, 1)

    whole(g_land, g_sem).wait()
    kv_copy.wait_recv()
    key_t[...] = kv_land[:, :head_dim].astype(jnp.float32).T.astype(jnp.bfloat16)

    def gq_copy(h, d):
        peer = lax.rem(me + d, n_seq)
        col = pl.multiple_of((me * heads + h) * head_dim, head_dim)
        row = pl.multiple_of(peer * tokens, tokens)
        return pltpu.make_async_remote_copy(
            src_ref=gq_buf.at[h, pl.ds(row, tokens), :],
            dst_ref=out_q.at[:, pl.ds(col, head_dim)],
            send_sem=gq_send_sem,
            recv_sem=gq_recv_sem,
            device_id=(section, peer),
            device_id_type=MESH,
        )

    def gq_self(h):
        col = pl.multiple_of((me * heads + h) * head_dim, head_dim)
        row = pl.multiple_of(me * tokens, tokens)
        return pltpu.make_async_copy(
            gq_buf.at[h, pl.ds(row, tokens), :],
            out_q.at[:, pl.ds(col, head_dim)],
            gq_recv_sem,
        )

    def kvp_target():
        if repeats == 1:
            width = 2 * head_dim
            return out_kv.at[:, pl.ds(pl.multiple_of(me * width, width), width)]
        return kv_slots.at[me]

    def kvp_copy(d):
        peer = lax.rem(me + d, n_seq)
        row = pl.multiple_of(peer * tokens, tokens)
        return pltpu.make_async_remote_copy(
            src_ref=kvp_buf.at[pl.ds(row, tokens), :],
            dst_ref=kvp_target(),
            send_sem=kvp_send_sem,
            recv_sem=kvp_recv_sem,
            device_id=(section, peer),
            device_id_type=MESH,
        )

    def kvp_self():
        row = pl.multiple_of(me * tokens, tokens)
        return pltpu.make_async_copy(
            kvp_buf.at[pl.ds(row, tokens), :], kvp_target(), kvp_recv_sem
        )

    def grads(h, start, stop):
        size = stop - start
        query = q_land[h, start:stop, :]
        grad = g_land[h, start:stop, :]
        score = dot_last(kv_land[:stop, :head_dim], query)
        dprob = dot_last(kv_land[:stop, head_dim:], grad)
        key_pos = lax.broadcasted_iota(jnp.int32, (size, size), 0)
        query_pos = lax.broadcasted_iota(jnp.int32, (size, size), 1)
        diag = jnp.where(key_pos <= query_pos, score[start:], -1e30)
        score = jnp.concatenate([score[:start], diag], axis=0) if start else diag
        top = jnp.max(score, axis=0, keepdims=True)
        expd = jnp.exp2((score - top) * (scale * math.log2(math.e)))
        inverse = 1.0 / jnp.sum(expd, axis=0, keepdims=True)
        prob = expd * inverse
        row_dot = jnp.sum(prob * dprob, axis=0, keepdims=True)
        dscore = (prob * (dprob - row_dot)).astype(jnp.bfloat16)
        weight = prob.astype(jnp.bfloat16)
        dv_acc[:stop, :] += dot_plain(weight, grad)
        dk_acc[:stop, :] += dot_plain(dscore, query)
        gq_t = dot_plain(key_t[:, :stop], dscore) * scale
        gq_buf[h, start:stop, :] = gq_t.T.astype(jnp.bfloat16)

    def send(copy_to, copy_self, start, stop):
        low, high = start // tokens, stop // tokens
        for d in range(1, n_seq):
            peer = lax.rem(me + d, n_seq)

            @pl.when(jnp.logical_and(peer >= low, peer < high))
            def _():
                copy_to(d).start()

        @pl.when(jnp.logical_and(me >= low, me < high))
        def _():
            copy_self().start()

    def send_gq(h, start, stop):
        send(functools.partial(gq_copy, h), functools.partial(gq_self, h), start, stop)

    def send_kvp(start, stop):
        rows = slice(start, stop)
        kvp_buf[rows, :head_dim] = (dk_acc[rows, :] * scale).astype(jnp.bfloat16)
        kvp_buf[rows, head_dim:] = dv_acc[rows, :].astype(jnp.bfloat16)
        send(kvp_copy, kvp_self, start, stop)

    def head_step(h, carry):
        q_copy(h).wait_recv()
        send_unit(h + ahead)
        for start in range(0, span, block_len):
            grads(h, start, start + block_len)
        send_gq(h, 0, span)
        return carry

    lax.fori_loop(0, last, head_step, 0)
    for part, (start, stop) in enumerate(parts):
        q_copy(last, part).wait_recv()
        for low in range(start // block_len * block_len, stop, block_len):
            grads(last, max(low, start), min(low + block_len, stop))
        send_kvp(start, stop)
        send_gq(last, start, stop)

    away = span - tokens
    whole(q_land, q_send_sem).wait()
    kv_copy.wait_send()
    whole(gq_buf.at[:, :away], gq_send_sem).wait()
    whole(kvp_buf.at[:away], kvp_send_sem).wait()
    whole(out_q, gq_recv_sem).wait()
    landed = out_kv if repeats == 1 else kv_slots
    whole(landed, kvp_recv_sem).wait()
    if repeats > 1:
        for j in range(kv_heads):
            total = kv_slots[j * repeats].astype(jnp.float32)
            for i in range(1, repeats):
                total = total + kv_slots[j * repeats + i].astype(jnp.float32)
            width = 2 * head_dim
            out_kv[:, j * width : (j + 1) * width] = total.astype(jnp.bfloat16)


def store_kernel(grad_q, grad_kv, out_q, out_kv, kv_rows, q_sem, kv_sem):
    store_q = pltpu.make_async_copy(grad_q, out_q, q_sem)
    store_q.start()
    width = kv_rows.shape[2]
    for j in range(kv_rows.shape[1]):
        kv_rows[:, j, :] = grad_kv[:, j * width : (j + 1) * width]
    store_kv = pltpu.make_async_copy(kv_rows, out_kv, kv_sem)
    store_kv.start()
    store_q.wait()
    store_kv.wait()


def on_device(n_section, n_seq, held_q, held_kv, grad_out):
    held_q, held_kv, grad_out = held_q[0], held_kv[0], grad_out[0]
    span, width = held_q.shape
    kv_heads = held_kv.shape[1]
    head_dim = held_kv.shape[2] // 2
    heads = width // head_dim
    block_len = min(128, span)
    tokens = span // n_seq
    repeats = n_seq // kv_heads
    bf16 = jnp.bfloat16
    slots = n_seq if repeats > 1 else 1
    hbm = pl.BlockSpec(memory_space=pltpu.HBM)
    vmem = pl.BlockSpec(memory_space=pltpu.VMEM)
    dma = pltpu.SemaphoreType.DMA
    grad_q, grad_kv = pl.pallas_call(
        functools.partial(kernel, n_section, n_seq, kv_heads, head_dim, heads, block_len),
        out_shape=(
            pltpu.VMEM((tokens, n_seq * width), bf16),
            pltpu.VMEM((tokens, kv_heads * 2 * head_dim), bf16),
        ),
        in_specs=[hbm, hbm, hbm],
        out_specs=(vmem, vmem),
        scratch_shapes=[
            pltpu.VMEM((heads, span, head_dim), bf16),
            pltpu.VMEM(held_kv.shape, bf16),
            pltpu.VMEM((span, 2 * head_dim), bf16),
            pltpu.VMEM((span, 2 * head_dim), bf16),
            pltpu.VMEM((heads, span, head_dim), bf16),
            pltpu.VMEM((head_dim, span), bf16),
            pltpu.VMEM((span, head_dim), jnp.float32),
            pltpu.VMEM((span, head_dim), jnp.float32),
            pltpu.VMEM((heads, span, head_dim), bf16),
            pltpu.VMEM((span, 2 * head_dim), bf16),
            pltpu.VMEM((slots, tokens, 2 * head_dim), bf16),
            dma,
            dma((heads + 2,)),
            dma,
            dma,
            dma,
            dma,
            dma,
            dma,
            dma,
            dma,
            pltpu.SemaphoreType.REGULAR,
        ],
        compiler_params=pltpu.CompilerParams(
            collective_id=0, has_side_effects=True, vmem_limit_bytes=63 * 2**20
        ),
    )(held_q, held_kv, grad_out)
    kv_shape = (tokens, kv_heads, 2 * head_dim)
    grad_q, grad_kv = pl.pallas_call(
        store_kernel,
        out_shape=(
            jax.ShapeDtypeStruct(grad_q.shape, bf16),
            jax.ShapeDtypeStruct(kv_shape, bf16),
        ),
        in_specs=[vmem, vmem],
        out_specs=(hbm, hbm),
        scratch_shapes=[pltpu.VMEM(kv_shape, bf16), dma, dma],
        compiler_params=pltpu.CompilerParams(vmem_limit_bytes=4 * 2**20),
    )(grad_q, grad_kv)
    return grad_q[None], grad_kv[None]


def solution(mesh):
    return jax.shard_map(
        functools.partial(on_device, mesh.shape["section"], mesh.shape["seq"]),
        mesh=mesh,
        in_specs=(
            P("section", None, "seq"),
            P("section", None, None, None),
            P("section", None, "seq"),
        ),
        out_specs=(P("section", "seq", None), P("section", "seq", None, None)),
        check_vma=False,
    )
```

```python
import functools
import math

import jax
import jax.numpy as jnp
from jax import lax
from jax.experimental import pallas as pl
from jax.experimental.pallas import tpu as pltpu
from jax.sharding import PartitionSpec as P

MESH = pl.DeviceIdType.MESH
AHEAD = 7
SHIFT = 4
SPLIT = 4


def dot_last(left, right):
    return lax.dot_general(
        left, right, (((1,), (1,)), ((), ())), preferred_element_type=jnp.float32
    )


def dot_plain(left, right):
    return jnp.dot(left, right, preferred_element_type=jnp.float32)


def kernel(
    n_section,
    n_seq,
    kv_heads,
    head_dim,
    heads,
    block_len,
    held_q,
    held_kv,
    grad_out,
    out_q,
    out_kv,
    q_land,
    kv_all,
    kv_send,
    kv_help,
    kv_land,
    g_land,
    key_t,
    dk_acc,
    dv_acc,
    gq_buf,
    kvp_buf,
    kv_slots,
    q_send_sem,
    q_recv_sem,
    kv_send_sem,
    kv_recv_sem,
    help_send_sem,
    help_recv_sem,
    g_sem,
    load_sem,
    gq_send_sem,
    gq_recv_sem,
    kvp_send_sem,
    kvp_recv_sem,
    door,
):
    section = lax.axis_index("section")
    me = lax.axis_index("seq")
    partner = lax.rem(section + n_section // 2, n_section)
    repeats = n_seq // kv_heads
    own_head = me // repeats
    span = held_q.shape[0]
    tokens = span // n_seq
    scale = head_dim**-0.5

    kv_load = pltpu.make_async_copy(held_kv, kv_all, load_sem)
    kv_load.start()

    def whole(ref, sem):
        return pltpu.make_async_copy(ref, ref, sem)

    def grad_load(h):
        cols = pl.ds(pl.multiple_of(h * head_dim, head_dim), head_dim)
        return pltpu.make_async_copy(grad_out.at[:, cols], g_land.at[h], g_sem)

    half = n_seq // 2
    upper = me >= half
    lower = jnp.logical_not(upper)
    split = min(SPLIT, heads)
    plain = heads - split
    middle = span // 2
    units = heads + split
    groups = [(0, plain, 0), (plain, split, 1), (heads, split, 2)]

    def first_row(stage):
        low_rows = upper if stage == 1 else lower
        return pl.multiple_of(jnp.where(low_rows, 0, middle), middle)

    def q_copy(group, unit):
        base, _, stage = group
        h = unit - base + (plain if stage else 0)
        cols = pl.ds(pl.multiple_of(h * head_dim, head_dim), head_dim)
        rows = pl.ds(first_row(stage), middle) if stage else slice(0, span)
        return pltpu.make_async_remote_copy(
            src_ref=held_q.at[rows, cols],
            dst_ref=q_land.at[h, rows, :],
            send_sem=q_send_sem,
            recv_sem=q_recv_sem.at[unit],
            device_id=(partner, me),
            device_id_type=MESH,
        )

    shift = span * SHIFT // 256 * 16
    kept = span - shift

    def kv_copy(rows):
        return pltpu.make_async_remote_copy(
            src_ref=kv_send.at[:rows],
            dst_ref=kv_land.at[:rows],
            send_sem=kv_send_sem,
            recv_sem=kv_recv_sem,
            device_id=(partner, me),
            device_id_type=MESH,
        )

    help_copy = pltpu.make_async_remote_copy(
        src_ref=kv_help,
        dst_ref=kv_land.at[kept:],
        send_sem=help_send_sem,
        recv_sem=help_recv_sem,
        device_id=(partner, lax.rem(me + half, n_seq)),
        device_id_type=MESH,
    )

    def on_kv(act):
        @pl.when(upper)
        def _():
            act(kv_copy(kept))

        @pl.when(lower)
        def _():
            act(kv_copy(span))

    def send_unit(unit):
        for group in groups:
            base, count, _ = group

            @pl.when(jnp.logical_and(unit >= base, unit < base + count))
            def _():
                q_copy(group, unit).start()

    barrier = pltpu.get_barrier_semaphore()
    pl.semaphore_signal(barrier, inc=1, device_id=(partner, me), device_id_type=MESH)
    late = section >= n_section // 2
    early = jnp.logical_not(late)

    def signal_peers(sem):
        for d in range(1, n_seq):
            peer = lax.rem(me + d, n_seq)
            pl.semaphore_signal(
                sem, inc=1, device_id=(section, peer), device_id_type=MESH
            )

    @pl.when(early)
    def _():
        signal_peers(barrier)

    for h in range(heads):
        grad_load(h).start()
    dk_acc[...] = jnp.zeros_like(dk_acc)
    dv_acc[...] = jnp.zeros_like(dv_acc)
    pl.semaphore_wait(barrier, jnp.where(early, n_seq, 1))
    send_unit(0)
    kv_load.wait()
    for j in range(kv_heads):

        @pl.when(own_head == j)
        def _():
            kv_send[...] = kv_all[:, j, :]

    inner = jnp.logical_and(section >= n_section // 4, section < n_section - n_section // 4)
    outer = jnp.logical_not(inner)

    @pl.when(jnp.logical_or(outer, upper))
    def _():
        on_kv(lambda copy: copy.start())

    ahead = jnp.where(section >= n_section - n_section // 4, AHEAD, units)

    def first_sends(unit, carry):
        @pl.when(unit < ahead)
        def _():
            send_unit(unit)

        return carry

    @pl.when(upper)
    def _():
        lax.fori_loop(1, units, first_sends, 0)

    @pl.when(lower)
    def _():
        for j in range(kv_heads):

            @pl.when((me + half) // repeats == j)
            def _():
                kv_help[...] = kv_all[kept:, j, :]

    @pl.when(early)
    def _():
        signal_peers(door)
        pl.semaphore_wait(door, n_seq - 1)
        pl.semaphore_signal(door, inc=1, device_id=(partner, me), device_id_type=MESH)

    @pl.when(late)
    def _():
        pl.semaphore_wait(door, 1)

    @pl.when(lower)
    def _():
        help_copy.start()

        @pl.when(inner)
        def _():
            on_kv(lambda copy: copy.start())

        lax.fori_loop(1, units, first_sends, 0)

    whole(g_land, g_sem).wait()
    on_kv(lambda copy: copy.wait_recv())

    @pl.when(upper)
    def _():
        help_copy.wait_recv()

    key_t[...] = kv_land[:, :head_dim].astype(jnp.float32).T.astype(jnp.bfloat16)

    def gq_copy(h, d):
        peer = lax.rem(me + d, n_seq)
        col = pl.multiple_of((me * heads + h) * head_dim, head_dim)
        row = pl.multiple_of(peer * tokens, tokens)
        return pltpu.make_async_remote_copy(
            src_ref=gq_buf.at[h, pl.ds(row, tokens), :],
            dst_ref=out_q.at[:, pl.ds(col, head_dim)],
            send_sem=gq_send_sem,
            recv_sem=gq_recv_sem,
            device_id=(section, peer),
            device_id_type=MESH,
        )

    def gq_self(h):
        col = pl.multiple_of((me * heads + h) * head_dim, head_dim)
        row = pl.multiple_of(me * tokens, tokens)
        return pltpu.make_async_copy(
            gq_buf.at[h, pl.ds(row, tokens), :],
            out_q.at[:, pl.ds(col, head_dim)],
            gq_recv_sem,
        )

    def kvp_target():
        if repeats == 1:
            width = 2 * head_dim
            return out_kv.at[:, pl.ds(pl.multiple_of(me * width, width), width)]
        return kv_slots.at[me]

    def kvp_copy(d):
        peer = lax.rem(me + d, n_seq)
        row = pl.multiple_of(peer * tokens, tokens)
        return pltpu.make_async_remote_copy(
            src_ref=kvp_buf.at[pl.ds(row, tokens), :],
            dst_ref=kvp_target(),
            send_sem=kvp_send_sem,
            recv_sem=kvp_recv_sem,
            device_id=(section, peer),
            device_id_type=MESH,
        )

    def kvp_self():
        row = pl.multiple_of(me * tokens, tokens)
        return pltpu.make_async_copy(
            kvp_buf.at[pl.ds(row, tokens), :], kvp_target(), kvp_recv_sem
        )

    def grads(h, start, stop):
        size = stop - start
        query = q_land[h, start:stop, :]
        grad = g_land[h, start:stop, :]
        score = dot_last(kv_land[:stop, :head_dim], query)
        dprob = dot_last(kv_land[:stop, head_dim:], grad)
        key_pos = lax.broadcasted_iota(jnp.int32, (size, size), 0)
        query_pos = lax.broadcasted_iota(jnp.int32, (size, size), 1)
        diag = jnp.where(key_pos <= query_pos, score[start:], -1e30)
        score = jnp.concatenate([score[:start], diag], axis=0) if start else diag
        top = jnp.max(score, axis=0, keepdims=True)
        expd = jnp.exp2((score - top) * (scale * math.log2(math.e)))
        inverse = 1.0 / jnp.sum(expd, axis=0, keepdims=True)
        prob = expd * inverse
        row_dot = jnp.sum(prob * dprob, axis=0, keepdims=True)
        dscore = (prob * (dprob - row_dot)).astype(jnp.bfloat16)
        weight = prob.astype(jnp.bfloat16)
        dv_acc[:stop, :] += dot_plain(weight, grad)
        dk_acc[:stop, :] += dot_plain(dscore, query)
        gq_t = dot_plain(key_t[:, :stop], dscore) * scale
        gq_buf[h, start:stop, :] = gq_t.T.astype(jnp.bfloat16)

    def send(copy_to, copy_self, start, stop):
        low, high = start // tokens, stop // tokens
        for d in range(1, n_seq):
            peer = lax.rem(me + d, n_seq)

            @pl.when(jnp.logical_and(peer >= low, peer < high))
            def _():
                copy_to(d).start()

        @pl.when(jnp.logical_and(me >= low, me < high))
        def _():
            copy_self().start()

    def send_gq(h, start, stop):
        send(functools.partial(gq_copy, h), functools.partial(gq_self, h), start, stop)

    def send_kvp(start, stop):
        rows = slice(start, stop)
        kvp_buf[rows, :head_dim] = (dk_acc[rows, :] * scale).astype(jnp.bfloat16)
        kvp_buf[rows, head_dim:] = dv_acc[rows, :].astype(jnp.bfloat16)
        send(kvp_copy, kvp_self, start, stop)

    def rows_step(h, start, stop, done=None):
        for low in range(start, stop, block_len):
            grads(h, low, min(low + block_len, stop))
        if done is not None:
            done()
        send_gq(h, start, stop)

    def stage_step(h, stage, final):
        def after(when, start, stop):
            def done():
                @pl.when(jnp.logical_and(final, when))
                def _():
                    send_kvp(start, stop)

            return done

        @pl.when(first_row(stage) == 0)
        def _():
            rows_step(h, 0, middle, after(stage == 2, 0, middle))

        @pl.when(first_row(stage) == middle)
        def _():
            if stage == 1:
                rows_step(h, middle, span, after(True, middle, span))
            else:
                rows_step(h, middle, span, after(True, 0, span))

    for group in groups:
        base, count, stage = group

        def unit_step(unit, carry):
            q_copy(group, unit).wait_recv()
            send_unit(unit + ahead)
            if stage:
                stage_step(unit - base + plain, stage, unit == base + count - 1)
            else:
                rows_step(unit, 0, span)
            return carry

        lax.fori_loop(base, base + count, unit_step, 0)

    away = span - tokens
    whole(q_land, q_send_sem).wait()
    on_kv(lambda copy: copy.wait_send())

    @pl.when(lower)
    def _():
        help_copy.wait_send()

    whole(gq_buf.at[:, :away], gq_send_sem).wait()
    whole(kvp_buf.at[:away], kvp_send_sem).wait()
    whole(out_q, gq_recv_sem).wait()
    landed = out_kv if repeats == 1 else kv_slots
    whole(landed, kvp_recv_sem).wait()
    if repeats > 1:
        for j in range(kv_heads):
            total = kv_slots[j * repeats].astype(jnp.float32)
            for i in range(1, repeats):
                total = total + kv_slots[j * repeats + i].astype(jnp.float32)
            width = 2 * head_dim
            out_kv[:, j * width : (j + 1) * width] = total.astype(jnp.bfloat16)


def store_kernel(grad_q, grad_kv, out_q, out_kv, kv_rows, q_sem, kv_sem):
    store_q = pltpu.make_async_copy(grad_q, out_q, q_sem)
    store_q.start()
    width = kv_rows.shape[2]
    for j in range(kv_rows.shape[1]):
        kv_rows[:, j, :] = grad_kv[:, j * width : (j + 1) * width]
    store_kv = pltpu.make_async_copy(kv_rows, out_kv, kv_sem)
    store_kv.start()
    store_q.wait()
    store_kv.wait()


def on_device(n_section, n_seq, held_q, held_kv, grad_out):
    held_q, held_kv, grad_out = held_q[0], held_kv[0], grad_out[0]
    span, width = held_q.shape
    kv_heads = held_kv.shape[1]
    head_dim = held_kv.shape[2] // 2
    heads = width // head_dim
    block_len = min(128, span)
    tokens = span // n_seq
    repeats = n_seq // kv_heads
    bf16 = jnp.bfloat16
    slots = n_seq if repeats > 1 else 1
    hbm = pl.BlockSpec(memory_space=pltpu.HBM)
    vmem = pl.BlockSpec(memory_space=pltpu.VMEM)
    dma = pltpu.SemaphoreType.DMA
    grad_q, grad_kv = pl.pallas_call(
        functools.partial(kernel, n_section, n_seq, kv_heads, head_dim, heads, block_len),
        out_shape=(
            pltpu.VMEM((tokens, n_seq * width), bf16),
            pltpu.VMEM((tokens, kv_heads * 2 * head_dim), bf16),
        ),
        in_specs=[hbm, hbm, hbm],
        out_specs=(vmem, vmem),
        scratch_shapes=[
            pltpu.VMEM((heads, span, head_dim), bf16),
            pltpu.VMEM(held_kv.shape, bf16),
            pltpu.VMEM((span, 2 * head_dim), bf16),
            pltpu.VMEM((span * SHIFT // 256 * 16, 2 * head_dim), bf16),
            pltpu.VMEM((span, 2 * head_dim), bf16),
            pltpu.VMEM((heads, span, head_dim), bf16),
            pltpu.VMEM((head_dim, span), bf16),
            pltpu.VMEM((span, head_dim), jnp.float32),
            pltpu.VMEM((span, head_dim), jnp.float32),
            pltpu.VMEM((heads, span, head_dim), bf16),
            pltpu.VMEM((span, 2 * head_dim), bf16),
            pltpu.VMEM((slots, tokens, 2 * head_dim), bf16),
            dma,
            dma((heads + min(SPLIT, heads),)),
            dma,
            dma,
            dma,
            dma,
            dma,
            dma,
            dma,
            dma,
            dma,
            dma,
            pltpu.SemaphoreType.REGULAR,
        ],
        compiler_params=pltpu.CompilerParams(
            collective_id=0, has_side_effects=True, vmem_limit_bytes=63 * 2**20
        ),
    )(held_q, held_kv, grad_out)
    kv_shape = (tokens, kv_heads, 2 * head_dim)
    grad_q, grad_kv = pl.pallas_call(
        store_kernel,
        out_shape=(
            jax.ShapeDtypeStruct(grad_q.shape, bf16),
            jax.ShapeDtypeStruct(kv_shape, bf16),
        ),
        in_specs=[vmem, vmem],
        out_specs=(hbm, hbm),
        scratch_shapes=[pltpu.VMEM(kv_shape, bf16), dma, dma],
        compiler_params=pltpu.CompilerParams(vmem_limit_bytes=4 * 2**20),
    )(grad_q, grad_kv)
    return grad_q[None], grad_kv[None]


def solution(mesh):
    return jax.shard_map(
        functools.partial(on_device, mesh.shape["section"], mesh.shape["seq"]),
        mesh=mesh,
        in_specs=(
            P("section", None, "seq"),
            P("section", None, None, None),
            P("section", None, "seq"),
        ),
        out_specs=(P("section", "seq", None), P("section", "seq", None, None)),
        check_vma=False,
    )
```
